32 devices in a mesh: gx: 4 (over y, x), gy: 8 (over z, core).
Axes of the slice: x: 2, y: 2, z: 4, core: 2. Of those that a mesh axis runs over, the one named last changes fastest.
Arguments:
- velocity: float32 [2, 2048, 4096], P(None, 'gx', 'gy'), may hold values from -3 to 3
- stress: float32 [3, 2048, 4096], P(None, 'gx', 'gy'), may hold values from -3 to 3
- strength: float32 [2048, 4096], P('gx', 'gy'), may hold values from 0.5 to 4
- ice_mass: float32 [2048, 4096], P('gx', 'gy'), may hold values from 0.3 to 20, as said below
- wind_stress: float32 [2, 2048, 4096], P(None, 'gx', 'gy'), may hold values from -6 to 6
- current: float32 [2, 2048, 4096], P(None, 'gx', 'gy'), may hold values from -3 to 3
- ice_mask: int32 [2048, 4096], P('gx', 'gy'), may hold values from 0 to 1, as said below
- open_water: int32 [2048, 4096], P('gx', 'gy'), may hold values 0 or 1
Outputs:
- new_velocity: float32 [2, 2048, 4096], P(None, 'gx', 'gy')
- new_stress: float32 [3, 2048, 4096], P(None, 'gx', 'gy')
- residual: float32 [], replicated
- kinetic_energy: float32 [], replicated
The draws below stay inside these ranges and needn't reach their ends.
Inputs may be any that keep to these rules, and one draw needn't show every extreme that they name: `ice_mask`: 1 marks an ocean cell, 0 a land cell. `ice_mass`: positive everywhere.
All inputs are finite; a program needn't handle non-finite values. No bound on the sum of `open_water` on one device may be relied on, other than what follows from the above.
Results may differ from the reference program's by a relative error of at most 0.00002.
Values sent between devices are 32-bit elements; how exact they have to be, the bound alone decides.
A program may use at most 128 MiB of HBM per device.

```python
import math
import jax
import jax.numpy as jnp

ITERS = 4
NX = 2048
NY = 4096


def draw_ice_mass(key, part):
    row_ramp = 1.0 + 2.0 * jnp.arange(NX, dtype=jnp.float32) / NX
    col_ramp = 1.0 + 2.0 * jnp.arange(NY, dtype=jnp.float32) / NY
    ramp = row_ramp[:, None] * col_ramp[None, :]
    rough = jax.random.uniform(key, (NX, NY), jnp.float32, 0.6, 1.4)
    return (ramp * rough).astype(jnp.float32)


def draw_ice_mask(key, part):
    row_index = jnp.arange(NX, dtype=jnp.int32)[:, None]
    col_index = jnp.arange(NY, dtype=jnp.int32)[None, :]
    land_cells = jnp.zeros((NX, NY), jnp.int32)
    for number in range(8):
        key_a, key_b, key_c, key_d = jax.random.split(jax.random.fold_in(key, number + 11), 4)
        start_x = jax.random.randint(key_a, (), 0, NX)
        width_x = jax.random.randint(key_b, (), 1, max(NX // 4, 2))
        start_y = jax.random.randint(key_c, (), 0, NY)
        width_y = jax.random.randint(key_d, (), 1, max(NY // 4, 2))
        inside = (row_index >= start_x) & (row_index < start_x + width_x) & (col_index >= start_y) & (col_index < start_y + width_y)
        land_cells = jnp.maximum(land_cells, inside.astype(jnp.int32))
    speckle = (jax.random.randint(jax.random.fold_in(key, 97), (NX, NY), 0, 16) == 0).astype(jnp.int32)
    land_cells = jnp.maximum(land_cells, speckle)
    return (1 - land_cells).astype(jnp.int32)


def set_ends(entries, own_key, low, high):
    longest = entries.shape.index(max(entries.shape))
    spots = []
    for shift in (0, 1):
        where = [jax.random.randint(jax.random.fold_in(own_key, axis), (), 0, length) for axis, length in enumerate(entries.shape)]
        where[longest] = (where[longest] + shift) % entries.shape[longest]
        spots.append(tuple(where))
    return entries.at[spots[0]].set(low).at[spots[1]].set(high)


def levels(key, extent, shards, smallest, high):
    level, own = 1.0, jax.random.fold_in(key, 6)
    for dim, blocks in shards:
        heights = jnp.exp(jax.random.uniform(jax.random.fold_in(own, dim), (blocks,), jnp.float32, smallest / len(shards), high / len(shards)))
        level = level * jnp.repeat(heights, extent[dim] // blocks).reshape([-1 if axis == dim else 1 for axis in range(len(extent))])
    return level


def normal_values(rng, dims, deviation, most, cuts=(), kind=jnp.bfloat16):
    level = levels(rng, dims, cuts, -0.22, 0.18) if cuts else 1.0
    drawn = jax.random.normal(rng, dims, jnp.float32) * deviation * level
    return jnp.minimum(jnp.maximum(drawn, -most), most).astype(kind)


def setup_inputs(seed: int = 0) -> dict:
    key_of = jax.random.split(jax.random.key(seed), 9)
    velocity = normal_values(key_of[0], (2, NX, NY), 0.5, 3.0, ((1, 4), (2, 8)), jnp.float32)
    stress = normal_values(key_of[1], (3, NX, NY), 0.5, 3.0, ((1, 4), (2, 8)), jnp.float32)
    strength = jnp.clip(jnp.exp(math.log(4.0) - 2.0794415 * jax.random.uniform(key_of[2], (NX, NY), jnp.float32) ** levels(key_of[2], (NX, NY), ((0, 4), (1, 8)), -0.2, 0.2)), 0.5, 4.0)
    ice_mass = draw_ice_mass(jax.random.fold_in(key_of[8], 71), 0)
    wind_stress = normal_values(key_of[4], (2, NX, NY), 1.0, 6.0, ((1, 4), (2, 8)), jnp.float32)
    current = normal_values(key_of[5], (2, NX, NY), 0.5, 3.0, ((1, 4), (2, 8)), jnp.float32)
    ice_mask = draw_ice_mask(jax.random.fold_in(key_of[8], 71), 0)
    open_water = set_ends((jax.random.randint(key_of[7], (NX, NY), 0, 8) < 1).astype(jnp.int32), jax.random.fold_in(key_of[7], 1), 0, 1)
    return {"velocity": velocity, "stress": stress, "strength": strength, "ice_mass": ice_mass, "wind_stress": wind_stress, "current": current, "ice_mask": ice_mask, "open_water": open_water}


relax_rate = 0.8
ecc_square = 4.0
delta_floor = 0.05
time_step = 0.5
drag_coef = 1.0
coriolis = 0.3

def corner_diffs(values):
    along_x = (values[1:, 1:] + values[1:, :-1] - values[:-1, 1:] - values[:-1, :-1]) * 0.5
    along_y = (values[1:, 1:] + values[:-1, 1:] - values[1:, :-1] - values[:-1, :-1]) * 0.5
    return (along_x, along_y)

def update_stress(velocity, stress, pressure):
    du_dx, du_dy = corner_diffs(velocity[0])
    dv_dx, dv_dy = corner_diffs(velocity[1])
    divu = du_dx + dv_dy
    tension = du_dx - dv_dy
    shear = du_dy + dv_dx
    deform = jnp.sqrt(divu * divu + (tension * tension + shear * shear) / ecc_square + delta_floor * delta_floor)
    viscous = pressure / deform
    first = (stress[0] + relax_rate * viscous * (divu - deform)) / (1.0 + relax_rate)
    second = (stress[1] + relax_rate * viscous * tension / ecc_square) / (1.0 + relax_rate)
    third = (stress[2] + relax_rate * viscous * shear * 0.5 / ecc_square) / (1.0 + relax_rate)
    return jnp.stack([first, second, third])

def stress_force(stress):
    normal_x = 0.5 * (stress[0] + stress[1])
    normal_y = 0.5 * (stress[0] - stress[1])
    normal_x_dx, unused_x = corner_diffs(normal_x)
    unused_y, normal_y_dy = corner_diffs(normal_y)
    shear_dx, shear_dy = corner_diffs(stress[2])
    return (normal_x_dx + shear_dy, shear_dx + normal_y_dy)

def advance(velocity, force_x, force_y, ice_mass, wind_stress, current, ice_weight):
    inertia = ice_mass / time_step
    diagonal = inertia + drag_coef
    turning = ice_mass * coriolis
    rhs_u = inertia * velocity[0] + force_x + wind_stress[0] + drag_coef * current[0]
    rhs_v = inertia * velocity[1] + force_y + wind_stress[1] + drag_coef * current[1]
    determinant = diagonal * diagonal + turning * turning
    new_u = (diagonal * rhs_u + turning * rhs_v) / determinant * ice_weight
    new_v = (diagonal * rhs_v - turning * rhs_u) / determinant * ice_weight
    return jnp.stack([new_u, new_v])

def reference(velocity, stress, strength, ice_mass, wind_stress, current, ice_mask, open_water):
    ice_weight = ice_mask.astype(jnp.float32) * (1.0 - open_water.astype(jnp.float32))
    pressure = strength * ice_weight
    previous = velocity
    for subcycle in range(ITERS):
        padded = jnp.pad(velocity, ((0, 0), (1, 0), (1, 0)))
        stress = update_stress(padded, stress, pressure)
        force_x, force_y = stress_force(jnp.pad(stress, ((0, 0), (0, 1), (0, 1))))
        previous = velocity
        velocity = advance(velocity, force_x, force_y, ice_mass, wind_stress, current, ice_weight)
    change = velocity - previous
    residual = jnp.sum(ice_weight * (change[0] * change[0] + change[1] * change[1])) / (NX * NY)
    kinetic = 0.5 * jnp.sum(ice_mass * ice_weight * (velocity[0] * velocity[0] + velocity[1] * velocity[1])) / (NX * NY)
    return (velocity, stress, residual, kinetic)
```

```python
import functools

import jax
import jax.numpy as jnp
from jax import lax
from jax.experimental import pallas as pl
from jax.experimental.pallas import tpu as pltpu
from jax.sharding import PartitionSpec as P

ITERS = 4
relax_rate = 0.8
time_step = 0.5
drag_coef = 1.0
coriolis = 0.3
delta_floor = 0.05
MESH = pl.DeviceIdType.MESH

U, V, S1, S2, S12, PR, M, TX, TY, CA, CB = range(11)
NF = 11
PAD = 8
LANE = 128
DIRS = ((-1, 0), (1, 0), (0, -1), (0, 1), (-1, -1), (-1, 1), (1, -1), (1, 1))


def exchange_kernel(
    nx, ny, rows, cols,
    vel, stress, strength, mass, wind, current, mask, water,
    dyn, par,
    strength_v, mass_v, wind_v, current_v, mask_v, water_v,
    pack_l, pack_r, recv_l, recv_r,
    load_sem, row_send, row_recv, col_send, col_recv, cor_send, cor_recv,
):
    ix = lax.axis_index("gx")
    iy = lax.axis_index("gy")
    mid = cols - 2 * LANE
    pieces = (
        (0, rows, 0, LANE),
        (0, rows, cols - LANE, LANE),
        (0, 8, LANE, mid),
        (rows - 8, 8, LANE, mid),
        (8, rows - 16, LANE, mid),
    )

    def loads(p):
        r0, nr, c0, nc = pieces[p]
        src = (pl.ds(r0, nr), pl.ds(c0, nc))
        ext = (pl.ds(r0 + PAD, nr), pl.ds(c0, nc))
        both = (slice(None),)
        pairs = (
            (strength.at[src], strength_v.at[src]),
            (mass.at[src], mass_v.at[src]),
            (mask.at[src], mask_v.at[src]),
            (water.at[src], water_v.at[src]),
            (vel.at[both + src], dyn.at[(pl.ds(U, 2),) + ext]),
            (stress.at[both + src], dyn.at[(pl.ds(S1, 3),) + ext]),
            (wind.at[both + src], wind_v.at[both + src]),
            (current.at[both + src], current_v.at[both + src]),
        )
        return [
            pltpu.make_async_copy(a, b, load_sem.at[p * 8 + k])
            for k, (a, b) in enumerate(pairs)
        ]

    for p in range(5):
        for c in loads(p):
            c.start()

    def exists(d):
        return (ix + d[0] >= 0) & (ix + d[0] < nx) & (iy + d[1] >= 0) & (iy + d[1] < ny)

    def peer(d):
        return (ix + d[0], iy + d[1])

    barrier = pltpu.get_barrier_semaphore()
    for d in DIRS:
        @pl.when(exists(d))
        def _():
            pl.semaphore_signal(barrier, inc=1, device_id=peer(d), device_id_type=MESH)
    span = jnp.minimum(ix, 1) + jnp.minimum(nx - 1 - ix, 1) + 1
    breadth = jnp.minimum(iy, 1) + jnp.minimum(ny - 1 - iy, 1) + 1
    pl.semaphore_wait(barrier, span * breadth - 1)

    def prepare(r0, nr, c0, nc, step):
        def body(k, carry):
            r = pl.multiple_of(r0 + k * step, 8)
            src = (pl.ds(r, step), pl.ds(c0, nc))
            dst = (pl.ds(pl.multiple_of(r + PAD, 8), step), pl.ds(c0, nc))
            w = mask_v[src].astype(jnp.float32) * (1.0 - water_v[src].astype(jnp.float32))
            m = mass_v[src]
            inertia = m * (1.0 / time_step)
            diagonal = inertia + drag_coef
            turning = m * coriolis
            scale = (0.25 * w) / (diagonal * diagonal + turning * turning)
            par[(PR - 5,) + dst] = strength_v[src] * w * (relax_rate / (1.0 + relax_rate))
            par[(M - 5,) + dst] = inertia * 4.0
            par[(TX - 5,) + dst] = (wind_v[(0,) + src] + drag_coef * current_v[(0,) + src]) * 4.0
            par[(TY - 5,) + dst] = (wind_v[(1,) + src] + drag_coef * current_v[(1,) + src]) * 4.0
            par[(CA - 5,) + dst] = diagonal * scale
            par[(CB - 5,) + dst] = turning * scale
            return carry

        lax.fori_loop(0, nr // step, body, 0)

    for p in range(4):
        for c in loads(p):
            c.wait()
    prepare(0, rows, 0, LANE, 32)
    prepare(0, rows, cols - LANE, LANE, 32)
    prepare(0, 8, LANE, mid, 8)
    prepare(rows - 8, 8, LANE, mid, 8)

    def plane(f):
        return (dyn, f) if f < 5 else (par, f - 5)

    lane = lax.broadcasted_iota(jnp.int32, (8, LANE), 1)
    half = rows // 2

    def pack(k, carry):
        r = pl.multiple_of(k * 8, 8)
        for out, c0, base in ((pack_l, 0, 0), (pack_r, cols - LANE, 4)):
            acc = jnp.zeros((8, LANE), jnp.float32)
            for h in range(2):
                for f in range(NF):
                    ref, q = plane(f)
                    x = ref[q, pl.ds(pl.multiple_of(r + PAD + h * half, 8), 8), pl.ds(c0, LANE)]
                    at = 4 * f + 64 * h
                    x = pltpu.roll(x, (at + base) % LANE, axis=1) if (at + base) % LANE else x
                    acc = jnp.where((lane >= at) & (lane < at + 4), x, acc)
            out[pl.ds(r, 8), :] = acc
        return carry

    lax.fori_loop(0, half // 8, pack, 0)

    def sends(d):
        dx, dy = d
        k = DIRS.index(d)
        out = []
        if dy == 0:
            a = PAD if dx < 0 else rows
            b = rows + PAD if dx < 0 else 0
            for n, ref in enumerate((dyn, par)):
                out.append((
                    ref.at[:, pl.ds(a, 8), pl.ds(0, cols)],
                    ref.at[:, pl.ds(b, 8), pl.ds(0, cols)],
                    row_send.at[2 * k + n], row_recv.at[2 * k + n],
                ))
        else:
            src, dst = (pack_l, recv_r) if dy < 0 else (pack_r, recv_l)
            if dx == 0:
                out.append((src, dst.at[pl.ds(8, half), :], col_send.at[k - 2], col_recv.at[k - 2]))
            else:
                a = 0 if dx < 0 else half - 8
                b = half + 8 if dx < 0 else 0
                out.append((
                    src.at[pl.ds(a, 8), :], dst.at[pl.ds(b, 8), :],
                    cor_send.at[k - 4], cor_recv.at[k - 4],
                ))
        return [
            pltpu.make_async_remote_copy(
                src_ref=a, dst_ref=b, send_sem=s, recv_sem=r,
                device_id=peer(d), device_id_type=MESH,
            )
            for a, b, s, r in out
        ]

    for d in DIRS:
        @pl.when(exists(d))
        def _():
            for c in sends(d):
                c.start()

    @pl.when(ix == 0)
    def _():
        for ref in (dyn, par):
            ref[:, 0:8, 0:cols] = jnp.zeros((ref.shape[0], 8, cols), jnp.float32)

    @pl.when(ix == nx - 1)
    def _():
        for ref in (dyn, par):
            ref[:, rows + PAD : rows + 16, 0:cols] = jnp.zeros((ref.shape[0], 8, cols), jnp.float32)

    for dy, buf in ((-1, recv_l), (1, recv_r)):
        @pl.when(~exists((0, dy)))
        def _():
            buf[8 : half + 8, :] = jnp.zeros((half, LANE), jnp.float32)

        for dx, b in ((-1, 0), (1, half + 8)):
            @pl.when(~exists((dx, dy)))
            def _():
                buf[b : b + 8, :] = jnp.zeros((8, LANE), jnp.float32)

    for c in loads(4):
        c.wait()
    prepare(8, rows - 16, LANE, mid, 8)

    for d in DIRS:
        @pl.when(exists(d))
        def _():
            for c in sends((-d[0], -d[1])):
                c.wait_recv()
            for c in sends(d):
                c.wait_send()

    def unpack(r, src, h):
        left = recv_l[pl.ds(src, 8), :]
        right = recv_r[pl.ds(src, 8), :]
        for f in range(NF):
            at = 4 * f + 64 * h
            x = pltpu.roll(right, LANE - at, axis=1) if at else right
            y = pltpu.roll(left, (LANE - 4 - at) % LANE, axis=1) if (LANE - 4 - at) % LANE else left
            ref, q = plane(f)
            ref[q, pl.ds(r, 8), pl.ds(cols, LANE)] = jnp.where(
                lane < 4, x, jnp.where(lane >= LANE - 4, y, 0.0)
            )

    unpack(0, 0, 1)
    unpack(rows + PAD, half + 8, 0)

    def body(k, carry):
        s = pl.multiple_of(k * 8 + 8, 8)
        for h in range(2):
            unpack(pl.multiple_of(s + h * half, 8), s, h)
        return carry

    lax.fori_loop(0, half // 8, body, 0)


def roll(x, by, axis):
    return pltpu.roll(x, by % x.shape[axis], axis=axis)


def cycle_kernel(rows, cols, dyn, par, new_vel, new_stress, part, work, acc, sem):
    wide = cols + LANE
    blocks = (rows + 2 * PAD) // 8
    keep = 1.0 / (1.0 + relax_rate)
    sub = lax.broadcasted_iota(jnp.int32, (8, wide), 0)
    first, last = sub == 0, sub == 7
    acc[...] = jnp.zeros_like(acc)

    def at(k):
        return pl.ds(pl.multiple_of(k * 8, 8), 8)

    def do_stress(src, k, q0, r0):
        u, v = src[U, at(k), :], src[V, at(k), :]
        q, r = u + v, u - v
        q1, r1 = roll(q, 1, 0), roll(r, 1, 0)
        qa, ra = jnp.where(first, q0, q1), jnp.where(first, r0, r1)
        x, y = q - ra, r - qa
        z, w = q + ra, r + qa
        d = x + roll(y, 1, 1)
        t = y + roll(x, 1, 1)
        s = z - roll(w, 1, 1)
        e = d * d + 0.25 * (t * t + s * s) + 4.0 * delta_floor * delta_floor
        pr = par[PR - 5, at(k), :]
        g = pr * lax.rsqrt(e)
        s1 = src[S1, at(k), :] * keep + (g * d - pr)
        s2 = src[S2, at(k), :] * keep + (0.25 * g) * t
        s12 = src[S12, at(k), :] * keep + (0.125 * g) * s
        work[S1, at(k), :] = s1
        work[S2, at(k), :] = s2
        work[S12, at(k), :] = s12
        return q1, r1, s1 + s2, s1 - s2, s12 + s12

    def do_vel(src, k, n, m, h, nn, mm, hh, final):
        nb, mb, hb = (
            jnp.where(last, roll(b, -1, 0), roll(a, -1, 0)) for a, b in ((n, nn), (m, mm), (h, hh))
        )
        dn, sh, dh, sm = nb - n, hb + h, hb - h, mb + m
        fx = roll(dn + sh, -1, 1) + (dn - sh)
        fy = roll(dh + sm, -1, 1) + (dh - sm)
        u, v = src[U, at(k), :], src[V, at(k), :]
        mass = par[M - 5, at(k), :]
        ru = mass * u + (fx + par[TX - 5, at(k), :])
        rv = mass * v + (fy + par[TY - 5, at(k), :])
        a, b = par[CA - 5, at(k), :], par[CB - 5, at(k), :]
        nu, nv = a * ru + b * rv, a * rv - b * ru
        work[U, at(k), :] = nu
        work[V, at(k), :] = nv
        if final:
            du, dv = (nu - u)[:, :cols], (nv - v)[:, :cols]
            acc[0] += du * du + dv * dv
            acc[1] += (mass * (nu * nu + nv * nv))[:, :cols]

    zero = jnp.zeros((8, wide), jnp.float32)

    def sweep(src, lo, hi, carry, final):
        def body(k, c):
            q0, r0, n, m, h = c
            q1, r1, nn, mm, hh = do_stress(src, k, q0, r0)
            do_vel(src, k - 1, n, m, h, nn, mm, hh, final)
            return q1, r1, nn, mm, hh

        return lax.fori_loop(lo, hi, body, carry)

    def out_copies(r0, nr, k):
        ext = (pl.ds(r0 + PAD, nr), pl.ds(0, cols))
        own = (slice(None), pl.ds(r0, nr))
        return (
            pltpu.make_async_copy(work.at[(pl.ds(U, 2),) + ext], new_vel.at[own], sem.at[2 * k]),
            pltpu.make_async_copy(work.at[(pl.ds(S1, 3),) + ext], new_stress.at[own], sem.at[2 * k + 1]),
        )

    for cyc in range(ITERS - 1):
        src = dyn if cyc == 0 else work
        carry = do_stress(src, 0, zero, zero)
        carry = sweep(src, 1, blocks, carry, False)
        q1, r1, n, m, h = carry
        do_vel(src, blocks - 1, n, m, h, n, m, h, False)

    own = rows // 8
    cuts = 4
    per = own // cuts
    _, _, n, m, h = carry = do_stress(work, 0, zero, zero)
    carry = do_stress(work, 1, carry[0], carry[1])
    for c in range(cuts):
        carry = sweep(work, 2 + c * per, 2 + (c + 1) * per, carry, True)
        for cp in out_copies(c * per * 8, per * 8, c):
            cp.start()
    part[...] = jnp.zeros_like(part)
    part[0:1, :] = sum_lanes(acc[0], cols)
    part[1:2, :] = sum_lanes(acc[1], cols)
    for c in range(cuts):
        for cp in out_copies(c * per * 8, per * 8, c):
            cp.wait()


def sum_lanes(x, cols):
    t = x[:, 0:LANE]
    for c in range(LANE, cols, LANE):
        t = t + x[:, c : c + LANE]
    return jnp.sum(t, axis=0, keepdims=True)


def sum_kernel(nx, ny, scale, part, out, slots, send_sem, recv_sem):
    n = nx * ny
    me = lax.axis_index("gx") * ny + lax.axis_index("gy")

    def target(k):
        t = lax.rem(me + k, n)
        return (t // ny, lax.rem(t, ny))

    barrier = pltpu.get_barrier_semaphore()

    def greet(k, c):
        pl.semaphore_signal(barrier, inc=1, device_id=target(k), device_id_type=MESH)
        return c

    lax.fori_loop(1, n, greet, 0)
    pl.semaphore_wait(barrier, n - 1)

    def copy(k):
        return pltpu.make_async_remote_copy(
            src_ref=part, dst_ref=slots.at[me], send_sem=send_sem.at[k], recv_sem=recv_sem.at[k],
            device_id=target(k), device_id_type=MESH,
        )

    def start(k, c):
        copy(k).start()
        return c

    lax.fori_loop(1, n, start, 0)
    slots[pl.ds(me, 1)] = part[...][None]

    def wait(k, c):
        copy(k).wait()
        return c

    lax.fori_loop(1, n, wait, 0)
    total = jnp.sum(slots[...], axis=0)
    total = jnp.sum(total, axis=1, keepdims=True)
    out[...] = jnp.broadcast_to(total * scale, out.shape)


def per_device(nx, ny, velocity, stress, strength, ice_mass, wind, current, ice_mask, open_water):
    _, rows, cols = velocity.shape
    wide, tall, half = cols + LANE, rows + 2 * PAD, rows // 2
    f32, i32 = jnp.float32, jnp.int32
    hbm = pl.BlockSpec(memory_space=pl.ANY)
    vmem = pl.BlockSpec(memory_space=pltpu.VMEM)
    dma = pltpu.SemaphoreType.DMA
    dyn, par = pl.pallas_call(
        functools.partial(exchange_kernel, nx, ny, rows, cols),
        out_shape=(
            pltpu.VMEM((5, tall, wide), f32),
            pltpu.VMEM((6, tall, wide), f32),
        ),
        in_specs=[pl.BlockSpec(memory_space=pltpu.HBM)] * 8,
        out_specs=(vmem, vmem),
        scratch_shapes=[
            pltpu.VMEM((rows, cols), f32),
            pltpu.VMEM((rows, cols), f32),
            pltpu.VMEM((2, rows, cols), f32),
            pltpu.VMEM((2, rows, cols), f32),
            pltpu.VMEM((rows, cols), i32),
            pltpu.VMEM((rows, cols), i32),
            pltpu.VMEM((half, LANE), f32),
            pltpu.VMEM((half, LANE), f32),
            pltpu.VMEM((half + 16, LANE), f32),
            pltpu.VMEM((half + 16, LANE), f32),
            dma((40,)), dma((4,)), dma((4,)), dma((2,)), dma((2,)), dma((4,)), dma((4,)),
        ],
        compiler_params=pltpu.CompilerParams(
            collective_id=0, has_side_effects=True, vmem_limit_bytes=K1_VMEM
        ),
        name="exchange",
    )(
        *[
            pltpu.with_memory_space_constraint(x, pltpu.HBM)
            for x in (velocity, stress, strength, ice_mass, wind, current, ice_mask, open_water)
        ]
    )
    new_vel, new_stress, part = pl.pallas_call(
        functools.partial(cycle_kernel, rows, cols),
        out_shape=(
            jax.ShapeDtypeStruct(velocity.shape, f32),
            jax.ShapeDtypeStruct(stress.shape, f32),
            jax.ShapeDtypeStruct((8, LANE), f32),
        ),
        in_specs=[vmem, vmem],
        out_specs=(hbm, hbm, vmem),
        scratch_shapes=[
            pltpu.VMEM((5, tall, wide), f32),
            pltpu.VMEM((2, 8, cols), f32),
            dma((8,)),
        ],
        compiler_params=pltpu.CompilerParams(vmem_limit_bytes=K2_VMEM),
        name="subcycles",
    )(dyn, par)
    sums = pl.pallas_call(
        functools.partial(sum_kernel, nx, ny, 1.0 / (rows * nx * cols * ny)),
        out_shape=jax.ShapeDtypeStruct((8, LANE), f32),
        in_specs=[vmem],
        out_specs=vmem,
        scratch_shapes=[
            pltpu.VMEM((nx * ny, 8, LANE), f32),
            dma((nx * ny,)),
            dma((nx * ny,)),
        ],
        compiler_params=pltpu.CompilerParams(
            collective_id=1, has_side_effects=True, vmem_limit_bytes=4 << 20
        ),
        name="totals",
    )(part)
    return new_vel, new_stress, sums[0, 0], sums[1, 0] * 0.0625


K1_VMEM = 12 << 20
K2_VMEM = 12 << 20


def solution(mesh):
    two, three = P("gx", "gy"), P(None, "gx", "gy")
    return jax.shard_map(
        functools.partial(per_device, mesh.shape["gx"], mesh.shape["gy"]),
        mesh=mesh,
        in_specs=(three, three, two, two, three, three, two, two),
        out_specs=(three, three, P(), P()),
        check_vma=False,
    )
```

```python
import functools

import jax
import jax.numpy as jnp
from jax import lax
from jax.experimental import pallas as pl
from jax.experimental.pallas import tpu as pltpu
from jax.sharding import PartitionSpec as P

ITERS = 4
relax_rate = 0.8
time_step = 0.5
drag_coef = 1.0
coriolis = 0.3
delta_floor = 0.05
MESH = pl.DeviceIdType.MESH

U, V, S1, S2, S12, PR, M, TX, TY, CA, CB = range(11)
NF = 11
PAD = 8
LANE = 128
DIRS = ((-1, 0), (1, 0), (0, -1), (0, 1), (-1, -1), (-1, 1), (1, -1), (1, 1))


def exchange_kernel(
    nx, ny, rows, cols,
    vel, stress, strength, mass, wind, current, mask, water,
    dyn, par,
    strength_v, mass_v, wind_v, current_v, mask_v, water_v,
    pack_l, pack_r, recv_l, recv_r,
    load_sem, row_send, row_recv, col_send, col_recv, cor_send, cor_recv,
):
    ix = lax.axis_index("gx")
    iy = lax.axis_index("gy")
    mid = cols - 2 * LANE
    pieces = (
        (0, rows, 0, LANE),
        (0, rows, cols - LANE, LANE),
        (0, 8, LANE, mid),
        (rows - 8, 8, LANE, mid),
        (8, rows - 16, LANE, mid),
    )

    def loads(p):
        r0, nr, c0, nc = pieces[p]
        src = (pl.ds(r0, nr), pl.ds(c0, nc))
        ext = (pl.ds(r0 + PAD, nr), pl.ds(c0, nc))
        both = (slice(None),)
        pairs = (
            (strength.at[src], strength_v.at[src]),
            (mass.at[src], mass_v.at[src]),
            (mask.at[src], mask_v.at[src]),
            (water.at[src], water_v.at[src]),
            (vel.at[both + src], dyn.at[(pl.ds(U, 2),) + ext]),
            (stress.at[both + src], dyn.at[(pl.ds(S1, 3),) + ext]),
            (wind.at[both + src], wind_v.at[both + src]),
            (current.at[both + src], current_v.at[both + src]),
        )
        return [
            pltpu.make_async_copy(a, b, load_sem.at[p * 8 + k])
            for k, (a, b) in enumerate(pairs)
        ]

    for p in range(5):
        for c in loads(p):
            c.start()

    def exists(d):
        return (ix + d[0] >= 0) & (ix + d[0] < nx) & (iy + d[1] >= 0) & (iy + d[1] < ny)

    def peer(d):
        return (ix + d[0], iy + d[1])

    barrier = pltpu.get_barrier_semaphore()
    for d in DIRS:
        @pl.when(exists(d))
        def _():
            pl.semaphore_signal(barrier, inc=1, device_id=peer(d), device_id_type=MESH)
    span = jnp.minimum(ix, 1) + jnp.minimum(nx - 1 - ix, 1) + 1
    breadth = jnp.minimum(iy, 1) + jnp.minimum(ny - 1 - iy, 1) + 1
    pl.semaphore_wait(barrier, span * breadth - 1)

    def prepare(r0, nr, c0, nc, step):
        def body(k, carry):
            r = pl.multiple_of(r0 + k * step, 8)
            src = (pl.ds(r, step), pl.ds(c0, nc))
            dst = (pl.ds(pl.multiple_of(r + PAD, 8), step), pl.ds(c0, nc))
            w = mask_v[src].astype(jnp.float32) * (1.0 - water_v[src].astype(jnp.float32))
            m = mass_v[src]
            inertia = m * (1.0 / time_step)
            diagonal = inertia + drag_coef
            turning = m * coriolis
            scale = (0.25 * w) / (diagonal * diagonal + turning * turning)
            par[(PR - 5,) + dst] = strength_v[src] * w * (relax_rate / (1.0 + relax_rate))
            par[(M - 5,) + dst] = inertia * 4.0
            par[(TX - 5,) + dst] = (wind_v[(0,) + src] + drag_coef * current_v[(0,) + src]) * 4.0
            par[(TY - 5,) + dst] = (wind_v[(1,) + src] + drag_coef * current_v[(1,) + src]) * 4.0
            par[(CA - 5,) + dst] = diagonal * scale
            par[(CB - 5,) + dst] = turning * scale
            return carry

        lax.fori_loop(0, nr // step, body, 0)

    for p in range(4):
        for c in loads(p):
            c.wait()
    prepare(0, rows, 0, LANE, 32)
    prepare(0, rows, cols - LANE, LANE, 32)
    prepare(0, 8, LANE, mid, 8)
    prepare(rows - 8, 8, LANE, mid, 8)

    def plane(f):
        return (dyn, f) if f < 5 else (par, f - 5)

    lane = lax.broadcasted_iota(jnp.int32, (8, LANE), 1)
    half = rows // 2

    def pack(k, carry):
        r = pl.multiple_of(k * 8, 8)
        for out, c0, base in ((pack_l, 0, 0), (pack_r, cols - LANE, 4)):
            acc = jnp.zeros((8, LANE), jnp.float32)
            for h in range(2):
                for f in range(NF):
                    ref, q = plane(f)
                    x = ref[q, pl.ds(pl.multiple_of(r + PAD + h * half, 8), 8), pl.ds(c0, LANE)]
                    at = 4 * f + 64 * h
                    x = pltpu.roll(x, (at + base) % LANE, axis=1) if (at + base) % LANE else x
                    acc = jnp.where((lane >= at) & (lane < at + 4), x, acc)
            out[pl.ds(r, 8), :] = acc
        return carry


    def sends(d):
        dx, dy = d
        k = DIRS.index(d)
        out = []
        if dy == 0:
            a = PAD if dx < 0 else rows
            b = rows + PAD if dx < 0 else 0
            for n, ref in enumerate((dyn, par)):
                out.append((
                    ref.at[:, pl.ds(a, 8), pl.ds(0, cols)],
                    ref.at[:, pl.ds(b, 8), pl.ds(0, cols)],
                    row_send.at[2 * k + n], row_recv.at[2 * k + n],
                ))
        else:
            src, dst = (pack_l, recv_r) if dy < 0 else (pack_r, recv_l)
            if dx == 0:
                out.append((src, dst.at[pl.ds(8, half), :], col_send.at[k - 2], col_recv.at[k - 2]))
            else:
                a = 0 if dx < 0 else half - 8
                b = half + 8 if dx < 0 else 0
                out.append((
                    src.at[pl.ds(a, 8), :], dst.at[pl.ds(b, 8), :],
                    cor_send.at[k - 4], cor_recv.at[k - 4],
                ))
        return [
            pltpu.make_async_remote_copy(
                src_ref=a, dst_ref=b, send_sem=s, recv_sem=r,
                device_id=peer(d), device_id_type=MESH,
            )
            for a, b, s, r in out
        ]

    for d in DIRS[:2]:
        @pl.when(exists(d))
        def _():
            for c in sends(d):
                c.start()

    lax.fori_loop(0, half // 8, pack, 0)

    for d in DIRS[2:]:
        @pl.when(exists(d))
        def _():
            for c in sends(d):
                c.start()

    @pl.when(ix == 0)
    def _():
        for ref in (dyn, par):
            ref[:, 0:8, 0:cols] = jnp.zeros((ref.shape[0], 8, cols), jnp.float32)

    @pl.when(ix == nx - 1)
    def _():
        for ref in (dyn, par):
            ref[:, rows + PAD : rows + 16, 0:cols] = jnp.zeros((ref.shape[0], 8, cols), jnp.float32)

    for dy, buf in ((-1, recv_l), (1, recv_r)):
        @pl.when(~exists((0, dy)))
        def _():
            buf[8 : half + 8, :] = jnp.zeros((half, LANE), jnp.float32)

        for dx, b in ((-1, 0), (1, half + 8)):
            @pl.when(~exists((dx, dy)))
            def _():
                buf[b : b + 8, :] = jnp.zeros((8, LANE), jnp.float32)

    for c in loads(4):
        c.wait()
    prepare(8, rows - 16, LANE, mid, 8)

    for d in DIRS:
        @pl.when(exists(d))
        def _():
            for c in sends((-d[0], -d[1])):
                c.wait_recv()
            for c in sends(d):
                c.wait_send()

    def unpack(r, src, h):
        left = recv_l[pl.ds(src, 8), :]
        right = recv_r[pl.ds(src, 8), :]
        for f in range(NF):
            at = 4 * f + 64 * h
            x = pltpu.roll(right, LANE - at, axis=1) if at else right
            y = pltpu.roll(left, (LANE - 4 - at) % LANE, axis=1) if (LANE - 4 - at) % LANE else left
            ref, q = plane(f)
            ref[q, pl.ds(r, 8), pl.ds(cols, LANE)] = jnp.where(
                lane < 4, x, jnp.where(lane >= LANE - 4, y, 0.0)
            )

    unpack(0, 0, 1)
    unpack(rows + PAD, half + 8, 0)

    def body(k, carry):
        s = pl.multiple_of(k * 8 + 8, 8)
        for h in range(2):
            unpack(pl.multiple_of(s + h * half, 8), s, h)
        return carry

    lax.fori_loop(0, half // 8, body, 0)


def roll(x, by, axis):
    return pltpu.roll(x, by % x.shape[axis], axis=axis)


def cycle_kernel(
    rows, cols, dyn, par, new_vel, new_stress, part, vel_a, sig_a, vel_b, sig_b, acc, sem
):
    wide = cols + LANE
    blocks = (rows + 2 * PAD) // 8
    keep = 1.0 / (1.0 + relax_rate)
    sub = lax.broadcasted_iota(jnp.int32, (8, wide), 0)
    first, last = sub == 0, sub == 7
    acc[...] = jnp.zeros_like(acc)

    def at(k):
        return pl.ds(pl.multiple_of(k * 8, 8), 8)

    def sum_diff(vel, k):
        u, v = vel[0, at(k), :], vel[1, at(k), :]
        return u + v, u - v

    def do_stress(vel, sig, to, k, count):
        q, r = sum_diff(vel, jnp.maximum(k - 1, 0))
        q0, r0 = roll(q, 1, 0), roll(r, 1, 0)
        for i in range(count):
            here = at(k + i)
            q, r = sum_diff(vel, k + i)
            q1, r1 = roll(q, 1, 0), roll(r, 1, 0)
            qa, ra = jnp.where(first, q0, q1), jnp.where(first, r0, r1)
            q0, r0 = q1, r1
            x, y = q - ra, r - qa
            z, w = q + ra, r + qa
            d = x + roll(y, 1, 1)
            t = y + roll(x, 1, 1)
            s = z - roll(w, 1, 1)
            e = d * d + 0.25 * (t * t + s * s) + 4.0 * delta_floor * delta_floor
            pr = par[PR - 5, here, :]
            g = pr * lax.rsqrt(e)
            to[0, here, :] = sig[0, here, :] * keep + (g * d - pr)
            to[1, here, :] = sig[1, here, :] * keep + (0.25 * g) * t
            to[2, here, :] = sig[2, here, :] * keep + (0.125 * g) * s

    def normals(sig, k):
        s1, s2, s12 = sig[0, at(k), :], sig[1, at(k), :], sig[2, at(k), :]
        out = s1 + s2, s1 - s2, s12 + s12
        return out, [roll(x, -1, 0) for x in out]

    def do_vel(vel, sig, to, k, count, final):
        now, up = normals(sig, k)
        for i in range(count):
            here = at(k + i)
            later, up_later = normals(sig, jnp.minimum(k + i + 1, blocks - 1))
            n, m, h = now
            nb, mb, hb = (jnp.where(last, b, a) for a, b in zip(up, up_later))
            now, up = later, up_later
            dn, sh, dh, sm = nb - n, hb + h, hb - h, mb + m
            fx = roll(dn + sh, -1, 1) + (dn - sh)
            fy = roll(dh + sm, -1, 1) + (dh - sm)
            u, v = vel[0, here, :], vel[1, here, :]
            mass = par[M - 5, here, :]
            ru = mass * u + (fx + par[TX - 5, here, :])
            rv = mass * v + (fy + par[TY - 5, here, :])
            a, b = par[CA - 5, here, :], par[CB - 5, here, :]
            nu, nv = a * ru + b * rv, a * rv - b * ru
            to[0, here, :] = nu
            to[1, here, :] = nv
            if final:
                du, dv = (nu - u)[:, :cols], (nv - v)[:, :cols]
                acc[2 * i] += du * du + dv * dv
                acc[2 * i + 1] += (mass * (nu * nu + nv * nv))[:, :cols]

    def sweep(old, new, skip, lo, hi, final):
        def body(p, c):
            do_vel(old[0], new[1], new[0], 2 * (p - 2) + skip, 2, final)
            do_stress(old[0], old[1], new[1], 2 * p + skip, 2)
            return c

        lax.fori_loop(lo, hi, body, 0)

    def out_copies(r0, nr, k):
        ext = (slice(None), pl.ds(r0 + PAD, nr), pl.ds(0, cols))
        own = (slice(None), pl.ds(r0, nr))
        return (
            pltpu.make_async_copy(new[0].at[ext], new_vel.at[own], sem.at[2 * k]),
            pltpu.make_async_copy(new[1].at[ext], new_stress.at[own], sem.at[2 * k + 1]),
        )

    start = (dyn.at[0:2], dyn.at[2:5])
    bufs = ((vel_a, sig_a), (vel_b, sig_b))
    pairs = blocks // 2
    for cyc in range(ITERS - 1):
        old = start if cyc == 0 else bufs[(cyc - 1) % 2]
        new = bufs[cyc % 2]
        do_stress(*old, new[1], 0, 4)
        sweep(old, new, 0, 2, pairs, False)
        do_vel(old[0], new[1], new[0], blocks - 4, 4, False)

    old, new = bufs[(ITERS - 2) % 2], bufs[(ITERS - 1) % 2]
    cuts = 4
    per = (blocks - 2) // cuts
    do_stress(*old, new[1], 1, 4)
    for c in range(cuts):
        end = c == cuts - 1
        sweep(old, new, 1, 2 + c * per // 2, pairs - 1 if end else 2 + (c + 1) * per // 2, True)
        if end:
            do_stress(*old, new[1], blocks - 1, 1)
            for j in (5, 3):
                do_vel(old[0], new[1], new[0], blocks - j, 2, True)
        for cp in out_copies(c * per * 8, per * 8, c):
            cp.start()
    part[...] = jnp.zeros_like(part)
    part[0:1, :] = sum_lanes(acc[0] + acc[2], cols)
    part[1:2, :] = sum_lanes(acc[1] + acc[3], cols)
    for c in range(cuts):
        for cp in out_copies(c * per * 8, per * 8, c):
            cp.wait()


def sum_lanes(x, cols):
    t = x[:, 0:LANE]
    for c in range(LANE, cols, LANE):
        t = t + x[:, c : c + LANE]
    return jnp.sum(t, axis=0, keepdims=True)


def sum_kernel(nx, ny, scale, part, out, slots, send_sem, recv_sem):
    n = nx * ny
    me = lax.axis_index("gx") * ny + lax.axis_index("gy")

    def target(k):
        t = lax.rem(me + k, n)
        return (t // ny, lax.rem(t, ny))

    barrier = pltpu.get_barrier_semaphore()

    def greet(k, c):
        pl.semaphore_signal(barrier, inc=1, device_id=target(k), device_id_type=MESH)
        return c

    lax.fori_loop(1, n, greet, 0)
    pl.semaphore_wait(barrier, n - 1)

    def copy(k):
        return pltpu.make_async_remote_copy(
            src_ref=part, dst_ref=slots.at[me], send_sem=send_sem.at[k], recv_sem=recv_sem.at[k],
            device_id=target(k), device_id_type=MESH,
        )

    def start(k, c):
        copy(k).start()
        return c

    lax.fori_loop(1, n, start, 0)
    slots[pl.ds(me, 1)] = part[...][None]

    def wait(k, c):
        copy(k).wait()
        return c

    lax.fori_loop(1, n, wait, 0)
    total = jnp.sum(slots[...], axis=0)
    total = jnp.sum(total, axis=1, keepdims=True)
    out[...] = jnp.broadcast_to(total * scale, out.shape)


def per_device(nx, ny, velocity, stress, strength, ice_mass, wind, current, ice_mask, open_water):
    _, rows, cols = velocity.shape
    wide, tall, half = cols + LANE, rows + 2 * PAD, rows // 2
    f32, i32 = jnp.float32, jnp.int32
    hbm = pl.BlockSpec(memory_space=pl.ANY)
    vmem = pl.BlockSpec(memory_space=pltpu.VMEM)
    dma = pltpu.SemaphoreType.DMA
    dyn, par = pl.pallas_call(
        functools.partial(exchange_kernel, nx, ny, rows, cols),
        out_shape=(
            pltpu.VMEM((5, tall, wide), f32),
            pltpu.VMEM((6, tall, wide), f32),
        ),
        in_specs=[pl.BlockSpec(memory_space=pltpu.HBM)] * 8,
        out_specs=(vmem, vmem),
        scratch_shapes=[
            pltpu.VMEM((rows, cols), f32),
            pltpu.VMEM((rows, cols), f32),
            pltpu.VMEM((2, rows, cols), f32),
            pltpu.VMEM((2, rows, cols), f32),
            pltpu.VMEM((rows, cols), i32),
            pltpu.VMEM((rows, cols), i32),
            pltpu.VMEM((half, LANE), f32),
            pltpu.VMEM((half, LANE), f32),
            pltpu.VMEM((half + 16, LANE), f32),
            pltpu.VMEM((half + 16, LANE), f32),
            dma((40,)), dma((4,)), dma((4,)), dma((2,)), dma((2,)), dma((4,)), dma((4,)),
        ],
        compiler_params=pltpu.CompilerParams(
            collective_id=0, has_side_effects=True, vmem_limit_bytes=K1_VMEM
        ),
        name="exchange",
    )(
        *[
            pltpu.with_memory_space_constraint(x, pltpu.HBM)
            for x in (velocity, stress, strength, ice_mass, wind, current, ice_mask, open_water)
        ]
    )
    new_vel, new_stress, part = pl.pallas_call(
        functools.partial(cycle_kernel, rows, cols),
        out_shape=(
            jax.ShapeDtypeStruct(velocity.shape, f32),
            jax.ShapeDtypeStruct(stress.shape, f32),
            jax.ShapeDtypeStruct((8, LANE), f32),
        ),
        in_specs=[vmem, vmem],
        out_specs=(hbm, hbm, vmem),
        scratch_shapes=[
            pltpu.VMEM((2, tall, wide), f32),
            pltpu.VMEM((3, tall, wide), f32),
            pltpu.VMEM((2, tall, wide), f32),
            pltpu.VMEM((3, tall, wide), f32),
            pltpu.VMEM((4, 8, cols), f32),
            dma((8,)),
        ],
        compiler_params=pltpu.CompilerParams(vmem_limit_bytes=K2_VMEM),
        name="subcycles",
    )(dyn, par)
    sums = pl.pallas_call(
        functools.partial(sum_kernel, nx, ny, 1.0 / (rows * nx * cols * ny)),
        out_shape=jax.ShapeDtypeStruct((8, LANE), f32),
        in_specs=[vmem],
        out_specs=vmem,
        scratch_shapes=[
            pltpu.VMEM((nx * ny, 8, LANE), f32),
            dma((nx * ny,)),
            dma((nx * ny,)),
        ],
        compiler_params=pltpu.CompilerParams(
            collective_id=1, has_side_effects=True, vmem_limit_bytes=4 << 20
        ),
        name="totals",
    )(part)
    return new_vel, new_stress, sums[0, 0], sums[1, 0] * 0.0625


K1_VMEM = 12 << 20
K2_VMEM = 24 << 20


def solution(mesh):
    two, three = P("gx", "gy"), P(None, "gx", "gy")
    return jax.shard_map(
        functools.partial(per_device, mesh.shape["gx"], mesh.shape["gy"]),
        mesh=mesh,
        in_specs=(three, three, two, two, three, three, two, two),
        out_specs=(three, three, P(), P()),
        check_vma=False,
    )
```
